128 devices in a mesh: replica: 1, dp: 128 (over z, y, x, core).
Axes of the slice: x: 4, y: 4, z: 4, core: 2. Of those that a mesh axis runs over, the one named last changes fastest.
Arguments:
- x: bfloat16 [512, 896], P(('replica', 'dp'))
- lengths: int32 [512], P(('replica', 'dp'))
- cache: bfloat16 [2, 512, 512, 576], P(None, ('replica', 'dp'))
- w_q: bfloat16 [2, 896, 9216], replicated
- w_o: bfloat16 [2, 8192, 896], replicated
- expert_ids: int32 [2, 512, 8], P(None, ('replica', 'dp'))
- slots: int32 [2, 512, 8], P(None, ('replica', 'dp'))
- route_w: float32 [2, 512, 8], P(None, ('replica', 'dp'))
- w1_exp: bfloat16 [2, 256, 896, 256], P(None, 'dp')
- w3_exp: bfloat16 [2, 256, 896, 256], P(None, 'dp')
- w2_exp: bfloat16 [2, 256, 256, 896], P(None, 'dp')
- w1_sh: bfloat16 [2, 896, 256], P(None, None, 'dp')
- w3_sh: bfloat16 [2, 896, 256], P(None, None, 'dp')
- w2_sh: bfloat16 [2, 256, 896], P(None, 'dp')
Outputs:
- output: bfloat16 [512, 896], P(('replica', 'dp'))
All inputs are finite; a program needn't handle non-finite values.
Results may differ from the reference program's by a relative error of at most 0.02.
Values are sent between devices in bfloat16 or wider.
A program may use at most 1 GiB of HBM per device.

```python
import jax
import jax.numpy as jnp
from jax import lax

GROUP_SIZE = 128
BATCH_DEV = 4
SEQ_LEN = 512
D_MODEL = 896
NUM_HEADS = 16
EXPERTS = 256
TOP_K = 8
FF_EXPERT = 256
FF_SHARED = 256
CAPACITY = 1
LAYERS = 2
LATENT = 512
ROPE_DIM = 64

KV_DIM = LATENT + ROPE_DIM
TOKENS = GROUP_SIZE * BATCH_DEV
BUFFER_ROWS = EXPERTS * GROUP_SIZE * CAPACITY
ATT_SCALE = 1.0 / (192.0 ** 0.5)
NORM_EPS = 1e-6


def scaled_normal(key, shape, scale):
    return (jax.random.normal(key, shape, jnp.float32) * scale).astype(jnp.bfloat16)


def draw_routing(key):
    key_bias, key_score, key_hot = jax.random.split(key, 3)
    expert_bias = jax.random.randint(key_bias, (LAYERS, 1, EXPERTS), 0, 512)
    raw_score = jax.random.randint(key_score, (LAYERS, TOKENS, EXPERTS), 0, 1024) + expert_bias
    hot_expert = jax.random.randint(key_hot, (LAYERS, GROUP_SIZE, 1, 1), 0, EXPERTS)
    first_rows = jnp.arange(BATCH_DEV)[None, None, :, None] < CAPACITY
    forced = jnp.logical_and(first_rows, jnp.arange(EXPERTS)[None, None, None, :] == hot_expert)
    raw_score = raw_score + 4096 * forced.astype(jnp.int32).reshape(LAYERS, TOKENS, EXPERTS)
    ranked = raw_score * EXPERTS + jnp.arange(EXPERTS)
    expert_ids = lax.top_k(ranked, TOP_K)[1].astype(jnp.int32)
    member = (expert_ids[:, :, :, None] == jnp.arange(EXPERTS)).astype(jnp.int32)
    member = member.reshape(LAYERS, GROUP_SIZE, BATCH_DEV * TOP_K, EXPERTS)
    slot_rank = jnp.sum(jnp.cumsum(member, axis=2) * member, axis=-1) - 1
    slot_rank = slot_rank.reshape(LAYERS, TOKENS, TOP_K)
    slots = jnp.where(slot_rank < CAPACITY, slot_rank, -1).astype(jnp.int32)
    return expert_ids, slots


def setup_inputs(seed: int = 0, part: int = 0) -> dict:
    part_keys = jax.random.split(jax.random.fold_in(jax.random.key(seed), part), 5)
    weight_keys = jax.random.split(jax.random.key(seed + 1), 8)
    x = scaled_normal(part_keys[0], (TOKENS, D_MODEL), 1.0)
    lengths = jax.random.randint(part_keys[1], (TOKENS,), 1, SEQ_LEN + 1).at[0].set(SEQ_LEN).astype(jnp.int32)
    cache = scaled_normal(part_keys[2], (LAYERS, TOKENS, SEQ_LEN, KV_DIM), 1.0)
    expert_ids, slots = draw_routing(part_keys[3])
    route_w = jax.random.uniform(part_keys[4], (LAYERS, TOKENS, TOP_K), jnp.float32, 0.5, 1.5) * (3.0 / TOP_K)
    return dict(
        x=x,
        lengths=lengths,
        cache=cache,
        w_q=scaled_normal(weight_keys[0], (LAYERS, D_MODEL, NUM_HEADS * KV_DIM), 1.5 * D_MODEL ** -0.5),
        w_o=scaled_normal(weight_keys[1], (LAYERS, NUM_HEADS * LATENT, D_MODEL), (NUM_HEADS * LATENT) ** -0.5),
        expert_ids=expert_ids,
        slots=slots,
        route_w=route_w,
        w1_exp=scaled_normal(weight_keys[2], (LAYERS, EXPERTS, D_MODEL, FF_EXPERT), D_MODEL ** -0.5),
        w3_exp=scaled_normal(weight_keys[3], (LAYERS, EXPERTS, D_MODEL, FF_EXPERT), D_MODEL ** -0.5),
        w2_exp=scaled_normal(weight_keys[4], (LAYERS, EXPERTS, FF_EXPERT, D_MODEL), 1.5 * FF_EXPERT ** -0.5),
        w1_sh=scaled_normal(weight_keys[5], (LAYERS, D_MODEL, FF_SHARED), D_MODEL ** -0.5),
        w3_sh=scaled_normal(weight_keys[6], (LAYERS, D_MODEL, FF_SHARED), D_MODEL ** -0.5),
        w2_sh=scaled_normal(weight_keys[7], (LAYERS, FF_SHARED, D_MODEL), 2.0 * FF_SHARED ** -0.5),
    )


def rms_norm(values):
    vals32 = values.astype(jnp.float32)
    return vals32 * lax.rsqrt(jnp.mean(vals32 * vals32, axis=-1, keepdims=True) + NORM_EPS)


def attend_block(block_args):
    q_block, cache_block, len_block = block_args
    scores = jnp.einsum('bhc,btc->bht', q_block.astype(jnp.float32), cache_block.astype(jnp.float32)) * ATT_SCALE
    valid = jnp.arange(SEQ_LEN)[None, None, :] < len_block[:, None, None]
    probs = jax.nn.softmax(jnp.where(valid, scores, -jnp.inf), axis=-1)
    probs = probs.astype(jnp.bfloat16).astype(jnp.float32)
    return jnp.einsum('bht,btc->bhc', probs, cache_block[:, :, :LATENT].astype(jnp.float32))


def reference(x, lengths, cache, w_q, w_o, expert_ids, slots, route_w, w1_exp, w3_exp, w2_exp, w1_sh, w3_sh, w2_sh):
    owner_dev = jnp.arange(TOKENS) // BATCH_DEV
    len_blocks = lengths.reshape(GROUP_SIZE, BATCH_DEV)

    def layer_step(resid, layer_args):
        cache_l, w_q_l, w_o_l, ids_l, slot_l, gate_w, w1_e, w3_e, w2_e, w1_s, w3_s, w2_s = layer_args
        normed = rms_norm(resid).astype(jnp.bfloat16)
        queries = jnp.dot(normed, w_q_l, preferred_element_type=jnp.float32).astype(jnp.bfloat16)
        queries = queries.reshape(GROUP_SIZE, BATCH_DEV, NUM_HEADS, KV_DIM)
        attn = lax.map(attend_block, (queries, cache_l.reshape(GROUP_SIZE, BATCH_DEV, SEQ_LEN, KV_DIM), len_blocks))
        attn = attn.astype(jnp.bfloat16).reshape(TOKENS, NUM_HEADS * LATENT)
        resid = (resid.astype(jnp.float32) + jnp.dot(attn, w_o_l, preferred_element_type=jnp.float32)).astype(jnp.bfloat16)
        ffn_in = rms_norm(resid).astype(jnp.bfloat16)
        shared_gate = jnp.dot(ffn_in, w3_s, preferred_element_type=jnp.float32)
        shared_up = jnp.dot(ffn_in, w1_s, preferred_element_type=jnp.float32)
        shared_h = (jax.nn.silu(shared_gate) * shared_up).astype(jnp.bfloat16)
        shared_out = jnp.dot(shared_h, w2_s, preferred_element_type=jnp.float32)
        buf_rows = jnp.where(slot_l >= 0, ids_l * (GROUP_SIZE * CAPACITY) + owner_dev[:, None] * CAPACITY + slot_l, BUFFER_ROWS)
        copies = jnp.broadcast_to(ffn_in[:, None, :], (TOKENS, TOP_K, D_MODEL)).reshape(TOKENS * TOP_K, D_MODEL)
        buffer = jnp.zeros((BUFFER_ROWS, D_MODEL), jnp.bfloat16).at[buf_rows.reshape(-1)].set(copies, mode='drop')
        buffer = buffer.reshape(EXPERTS, GROUP_SIZE * CAPACITY, D_MODEL).astype(jnp.float32)
        gate_in = jnp.einsum('ecd,edf->ecf', buffer, w3_e.astype(jnp.float32))
        up_in = jnp.einsum('ecd,edf->ecf', buffer, w1_e.astype(jnp.float32))
        hidden = (jax.nn.silu(gate_in) * up_in).astype(jnp.bfloat16).astype(jnp.float32)
        expert_out = jnp.einsum('ecf,efd->ecd', hidden, w2_e.astype(jnp.float32)).astype(jnp.bfloat16)
        picked = jnp.take(expert_out.reshape(BUFFER_ROWS, D_MODEL), buf_rows, axis=0, mode='fill', fill_value=0)
        routed = jnp.sum(gate_w[:, :, None] * picked.astype(jnp.float32), axis=1)
        resid = (resid.astype(jnp.float32) + routed + shared_out).astype(jnp.bfloat16)
        return resid, None

    final_x = lax.scan(layer_step, x, (cache, w_q, w_o, expert_ids, slots, route_w, w1_exp, w3_exp, w2_exp, w1_sh, w3_sh, w2_sh))[0]
    return final_x
```

```python
import functools

import jax
import jax.numpy as jnp
from jax import lax
from jax.experimental import pallas as pl
from jax.experimental.pallas import tpu as pltpu
from jax.sharding import PartitionSpec as P

NORM_EPS = 1e-6
ATT_SCALE = 1.0 / (192.0 ** 0.5)
BF = jnp.bfloat16
F32 = jnp.float32
MESH = pl.DeviceIdType.MESH
DEPTH = 5


def grid_of(group):
    return (4, 4, group // 32, 2) if group >= 32 else (1, 1, group // 2, 2)


def rms(v):
    return v * lax.rsqrt(jnp.mean(v * v, axis=-1, keepdims=True) + NORM_EPS)


def nt_dot(a, b):
    return lax.dot_general(a, b, (((1,), (1,)), ((), ())), preferred_element_type=F32)


def dot(a, b):
    return jnp.dot(a, b, preferred_element_type=F32)


def kernel(
    group, nq, no,
    x_in, len_in, kv_in, wq_in, wo_in, ids_in, slot_in, rw_in, w1_in, w3_in, w2_in, w1s_in, w3s_in, w2s_in,
    out_ref,
    xb, len_s, ids_s, slot_s, rw_s, kv, wq, wo, w1, w3, w2, pack, sw,
    disp_out, disp_in, ret_out, ret_in, size, qflat, qs, osc, sel, place, gates,
    small_sem, kv_sem, wq_sem, wo_sem, ex_sem, pack_sem,
    ws_sem, wr_sem, fs_sem, fr_sem, ds_sem, dr_sem, rs_sem, rr_sem,
):
    layers, batch, kv_dim, seq = kv.shape
    d_model = xb.shape[1]
    heads = qs.shape[0]
    latent = osc.shape[2]
    top_k = ids_s.shape[2]
    experts = disp_out.shape[1]
    zs, ys, xs, cs = grid_of(group)
    half = group // cs * 2
    q_cols = wq.shape[2]
    o_rows = wo.shape[1]

    me = lax.axis_index("dp")
    my_core = me % cs
    my_x = (me // cs) % xs
    my_y = (me // (cs * xs)) % ys
    my_z = me // (cs * xs * ys)
    chip = me // cs

    def peer(i):
        core = (my_core + i) % cs
        px = (my_x + i // cs) % xs
        py = (my_y + i // (cs * xs)) % ys
        pz = (my_z + i // (cs * xs * ys)) % zs
        return ((pz * ys + py) * xs + px) * cs + core

    smalls = [
        pltpu.make_async_copy(src, dst, small_sem.at[i])
        for i, (src, dst) in enumerate(
            ((x_in, xb), (len_in, len_s), (ids_in, ids_s), (slot_in, slot_s), (rw_in, rw_s))
        )
    ]
    packs = [pltpu.make_async_copy(src, pack.at[:, i], pack_sem.at[i]) for i, src in enumerate((w1s_in, w3s_in, w2s_in))]

    def q_copy(layer, c):
        return pltpu.make_async_copy(wq_in.at[layer, :, pl.ds(c * q_cols, q_cols)], wq.at[c], wq_sem.at[c])

    def o_copy(layer, c):
        return pltpu.make_async_copy(wo_in.at[layer, pl.ds(c * o_rows, o_rows)], wo.at[c], wo_sem.at[c])

    def kv_copy(layer, b):
        return pltpu.make_async_copy(kv_in.at[layer, b], kv.at[layer, b], kv_sem.at[layer, b])

    def ex_copies(layer):
        return [
            pltpu.make_async_copy(src.at[layer], dst.at[layer], ex_sem.at[layer, i])
            for i, (src, dst) in enumerate(((w3_in, w3), (w1_in, w1), (w2_in, w2)))
        ]

    for cp in smalls:
        cp.start()
    stream = [q_copy(0, c) for c in range(nq)] + [kv_copy(0, b) for b in range(batch)]
    stream += [o_copy(0, c) for c in range(no)] + ex_copies(0)
    issued = [0]

    def issue(n):
        for _ in range(n):
            if issued[0] < len(stream):
                stream[issued[0]].start()
                issued[0] += 1

    issue(DEPTH)
    for cp in packs:
        cp.start()

    barrier = pltpu.get_barrier_semaphore()

    def signal(i, carry):
        pl.semaphore_signal(barrier, inc=1, device_id={"dp": peer(i)}, device_id_type=MESH)
        return carry

    lax.fori_loop(1, group, signal, 0)

    for cp in smalls:
        cp.wait()
    pairs = batch * top_k
    row = lax.broadcasted_iota(jnp.int32, (pairs, 1), 0)
    grow = lax.broadcasted_iota(jnp.int32, (pairs, 128), 0)
    erow = lax.broadcasted_iota(jnp.int32, (pairs, experts), 1)
    for layer in range(layers):
        ids = jnp.full((pairs, 1), -1, jnp.int32)
        gate = jnp.zeros((pairs, 128), F32)
        for t in range(batch):
            for j in range(top_k):
                kept = jnp.where(slot_s[layer, t, j] >= 0, ids_s[layer, t, j], -1)
                ids = jnp.where(row == t * top_k + j, kept, ids)
                gate = jnp.where(grow == t * top_k + j, rw_s[layer, t, j], gate)
        hot = jnp.where(erow == ids, 1.0, 0.0)
        sel[layer] = hot.astype(BF)
        gates[layer] = gate
        tok = jnp.sum(hot.reshape(batch, top_k, experts), axis=1)
        tok = jnp.concatenate([tok, jnp.zeros((128 - batch, experts), F32)], axis=0)
        place[layer] = tok.T.astype(BF)
    osc[...] = jnp.zeros(osc.shape, F32)

    col = lax.broadcasted_iota(jnp.int32, (heads, seq), 1)
    odd = lax.broadcasted_iota(jnp.int32, (experts, w1.shape[3]), 0) % 2
    resid = jnp.concatenate([xb[...].astype(F32), jnp.zeros((8 - batch, d_model), F32)], axis=0)

    def share(layer):
        def send(i, carry):
            dst = peer(i * cs)
            pltpu.make_async_remote_copy(
                src_ref=pack.at[layer],
                dst_ref=sw.at[layer, :, pl.ds(pl.multiple_of(my_core * half + chip * 2, 2), 2)],
                send_sem=ws_sem.at[layer], recv_sem=wr_sem.at[layer],
                device_id={"dp": dst}, device_id_type=MESH,
            ).start()
            return carry

        lax.fori_loop(1, group // cs, send, 0)
        for i, src in enumerate((w1s_in, w3s_in, w2s_in)):
            own = sw.at[layer, i, pl.ds(pl.multiple_of(my_core * half + chip * 2, 2), 2)]
            pltpu.make_async_copy(src.at[layer], own, wr_sem.at[layer]).start()

    def share_wait(layer):
        part = size.at[pl.ds(0, 3 * (group // cs - 1))]
        pltpu.make_async_remote_copy(
            src_ref=part, dst_ref=part, send_sem=ws_sem.at[layer], recv_sem=wr_sem.at[layer],
            device_id={"dp": me}, device_id_type=MESH,
        ).wait_send()
        part = sw.at[layer, :, pl.ds(0, half)]
        pltpu.make_async_remote_copy(
            src_ref=part, dst_ref=part, send_sem=ws_sem.at[layer], recv_sem=wr_sem.at[layer],
            device_id={"dp": me}, device_id_type=MESH,
        ).wait_recv()

    def forward(layer):
        mine = sw.at[layer, :, pl.ds(pl.multiple_of(my_core * half, 8), half)]
        return pltpu.make_async_remote_copy(
            src_ref=mine, dst_ref=mine, send_sem=fs_sem.at[layer], recv_sem=fr_sem.at[layer],
            device_id={"dp": chip * cs + (cs - 1 - my_core)}, device_id_type=MESH,
        )

    def exchange(src, dst, layer, send_sem, recv_sem):
        def send(i, carry):
            to = peer(i)
            pltpu.make_async_remote_copy(
                src_ref=src.at[layer, pl.ds(pl.multiple_of(to * 2, 2), 2)],
                dst_ref=dst.at[layer, pl.ds(pl.multiple_of(me * 2, 2), 2)],
                send_sem=send_sem.at[layer], recv_sem=recv_sem.at[layer],
                device_id={"dp": to}, device_id_type=MESH,
            ).start()
            return carry

        lax.fori_loop(1, group, send, 0)
        own = pl.ds(pl.multiple_of(me * 2, 2), 2)
        pltpu.make_async_copy(src.at[layer, own], dst.at[layer, own], recv_sem.at[layer]).start()

    def exchange_done(dst, layer, send_sem, recv_sem):
        part = size.at[pl.ds(0, group - 1)]
        pltpu.make_async_remote_copy(
            src_ref=part, dst_ref=part, send_sem=send_sem.at[layer], recv_sem=recv_sem.at[layer],
            device_id={"dp": me}, device_id_type=MESH,
        ).wait_send()
        pltpu.make_async_remote_copy(
            src_ref=dst.at[layer], dst_ref=dst.at[layer], send_sem=send_sem.at[layer], recv_sem=recv_sem.at[layer],
            device_id={"dp": me}, device_id_type=MESH,
        ).wait_recv()

    for layer in range(layers):
        h = rms(resid).astype(BF)
        for c in range(nq):
            q_copy(layer, c).wait()
            qflat[:, c * q_cols:(c + 1) * q_cols] = dot(h, wq[c])
            issue(1)
        for hd in range(heads):
            lo = hd * kv_dim
            base = lo // 128 * 128
            wide = qflat[:, base:base + -(-(lo - base + kv_dim) // 128) * 128]
            qs[hd] = wide[:, lo - base:lo - base + kv_dim]
        if layer == 0:
            pl.semaphore_wait(barrier, group - 1)
            for cp in packs:
                cp.wait()
        share(layer)
        for b in range(batch):
            kv_copy(layer, b).wait()
            s = dot(qs[:, b, :].astype(BF), kv[layer, b]) * ATT_SCALE
            s = jnp.where(col < len_s[b], s, -jnp.inf)
            e = jnp.exp(s - jnp.max(s, axis=-1, keepdims=True))
            p = (e / jnp.sum(e, axis=-1, keepdims=True)).astype(BF)
            osc[b] = nt_dot(p, kv[layer, b, 0:latent, :])
            issue(1)
        acc = jnp.zeros((8, d_model), F32)
        for c in range(no):
            o_copy(layer, c).wait()
            for i in range(o_rows // latent):
                hd = c * (o_rows // latent) + i
                acc += dot(osc[:, hd, :].astype(BF), wo[c, i * latent:(i + 1) * latent])
            issue(1)
        resid = (resid + acc).astype(BF).astype(F32)
        g32 = rms(resid).astype(BF).astype(F32)
        g = g32.astype(BF)
        gpad = jnp.concatenate([g32, jnp.zeros((120, d_model), F32)], axis=0).astype(BF)
        disp_out[layer] = dot(place[layer], gpad).astype(BF)
        exchange(disp_out, disp_in, layer, ds_sem, dr_sem)
        if layer == 0:
            issue(len(stream))
            for cp in [kv_copy(1, b) for b in range(batch)] + ex_copies(1):
                cp.start()
            for c in range(nq):
                q_copy(1, c).start()
            for c in range(no):
                o_copy(1, c).start()
        share_wait(layer)
        fwd = forward(layer)
        fwd.start()
        for cp in ex_copies(layer):
            cp.wait()
        fwd.wait()
        gate_in = nt_dot(g, sw[layer, 1])
        up_in = nt_dot(g, sw[layer, 0])
        shared = dot((jax.nn.silu(gate_in) * up_in).astype(BF), sw[layer, 2])
        exchange_done(disp_in, layer, ds_sem, dr_sem)
        toks = disp_in[layer]
        u = None
        for n in range(2):
            gate_in = dot(toks, w3[layer, n])
            up_in = dot(toks, w1[layer, n])
            hid = jnp.where(odd == n, jax.nn.silu(gate_in) * up_in, 0.0).astype(BF)
            part = dot(hid, w2[layer, n])
            u = part if u is None else u + part
        ret_out[layer] = u.astype(BF)
        exchange(ret_out, ret_in, layer, rs_sem, rr_sem)
        exchange_done(ret_in, layer, rs_sem, rr_sem)
        picked = dot(sel[layer], ret_in[layer])
        gate = gates[layer]
        picked = picked * jnp.concatenate([gate] * (d_model // 128), axis=1)
        routed = jnp.sum(picked.reshape(batch, top_k, d_model), axis=1)
        routed = jnp.concatenate([routed, jnp.zeros((8 - batch, d_model), F32)], axis=0)
        resid = (resid + routed + shared).astype(BF).astype(F32)
    out_ref[...] = resid[0:batch].astype(BF)


def solution(mesh):
    group = mesh.shape['dp']
    tok_axes = ('replica', 'dp')
    in_specs = (
        P(tok_axes, None), P(tok_axes), P(None, tok_axes, None, None),
        P(None, None, None), P(None, None, None),
        P(None, tok_axes, None), P(None, tok_axes, None), P(None, tok_axes, None),
        P(None, 'dp', None, None), P(None, 'dp', None, None), P(None, 'dp', None, None),
        P(None, None, 'dp'), P(None, None, 'dp'), P(None, 'dp', None),
    )

    def device_step(x, lengths, cache, w_q, w_o, expert_ids, slots, route_w, w1_exp, w3_exp, w2_exp, w1_sh, w3_sh, w2_sh):
        batch, d_model = x.shape
        layers, _, seq, kv_dim = cache.shape
        top_k = expert_ids.shape[2]
        experts = w1_exp.shape[1] * group
        heads = w_q.shape[2] // kv_dim
        latent = w_o.shape[1] // heads
        q_cols = 1024 if w_q.shape[2] % 1024 == 0 else 256
        o_rows = 2 * latent
        nq, no = w_q.shape[2] // q_cols, w_o.shape[1] // o_rows
        kv_t = jnp.swapaxes(cache, 2, 3)
        w1s_t = jnp.swapaxes(w1_sh, 1, 2)
        w3s_t = jnp.swapaxes(w3_sh, 1, 2)
        args = (x, lengths, kv_t, w_q, w_o, expert_ids, slots, route_w, w1_exp, w3_exp, w2_exp, w1s_t, w3s_t, w2_sh)
        dma = pltpu.SemaphoreType.DMA
        return pl.pallas_call(
            functools.partial(kernel, group, nq, no),
            out_shape=jax.ShapeDtypeStruct((batch, d_model), BF),
            in_specs=[pl.BlockSpec(memory_space=pl.ANY)] * len(args),
            out_specs=pl.BlockSpec(memory_space=pltpu.VMEM),
            scratch_shapes=[
                pltpu.VMEM((batch, d_model), BF),
                pltpu.SMEM(lengths.shape, jnp.int32),
                pltpu.SMEM(expert_ids.shape, jnp.int32),
                pltpu.SMEM(slots.shape, jnp.int32),
                pltpu.SMEM(route_w.shape, F32),
                pltpu.VMEM(kv_t.shape, BF),
                pltpu.VMEM((nq, d_model, q_cols), BF),
                pltpu.VMEM((no, o_rows, d_model), BF),
                pltpu.VMEM(w1_exp.shape, BF),
                pltpu.VMEM(w3_exp.shape, BF),
                pltpu.VMEM(w2_exp.shape, BF),
                pltpu.VMEM((layers, 3, 2, d_model), BF),
                pltpu.VMEM((layers, 3, 2 * group, d_model), BF),
                pltpu.VMEM((layers, experts, d_model), BF),
                pltpu.VMEM((layers, experts, d_model), BF),
                pltpu.VMEM((layers, experts, d_model), BF),
                pltpu.VMEM((layers, experts, d_model), BF),
                pltpu.VMEM((3 * group // 2, 2, d_model), BF),
                pltpu.VMEM((8, w_q.shape[2]), F32),
                pltpu.VMEM((heads, 8, kv_dim), F32),
                pltpu.VMEM((8, heads, latent), F32),
                pltpu.VMEM((layers, batch * top_k, experts), BF),
                pltpu.VMEM((layers, experts, 128), BF),
                pltpu.VMEM((layers, batch * top_k, 128), F32),
                dma((5,)), dma((layers, batch)), dma((nq,)), dma((no,)), dma((layers, 3)), dma((3,)),
                dma((layers,)), dma((layers,)), dma((layers,)), dma((layers,)),
                dma((layers,)), dma((layers,)), dma((layers,)), dma((layers,)),
            ],
            compiler_params=pltpu.CompilerParams(
                collective_id=0, has_side_effects=True, vmem_limit_bytes=60 * 1024 * 1024
            ),
        )(*args)

    return jax.shard_map(device_step, mesh=mesh, in_specs=in_specs, out_specs=P(tok_axes, None), check_vma=False)
```
